32 devices in a mesh: grp: 2 (over y), tgt: 4 (over z), src: 4 (over x, core).
Axes of the slice: x: 2, y: 2, z: 4, core: 2. Of those that a mesh axis runs over, the one named last changes fastest.
Arguments:
- target_rows: bfloat16 [2048, 4608], P(('grp', 'tgt', 'src')), parts along dimension 0, may hold values from -6 to 6
- target_pos: int32 [2048], P(('grp', 'tgt')), parts along dimension 0, may hold values from 0 to 255
- decoder_rows: bfloat16 [512, 4608], P(('grp', 'tgt', 'src')), parts along dimension 0, may hold values from -0.09375 to 0.09375
- source_pos: int32 [512], P('grp'), parts along dimension 0, may hold values from 0 to 255
- out_proj: bfloat16 [32, 4608, 128], P('src', 'tgt'), may hold values from -0.09375 to 0.09375
- value_proj: bfloat16 [16, 4608, 128], P('src'), may hold values from -1 to 1
- attention: bfloat16 [64, 256, 256], P(('grp', 'src'), 'tgt'), parts along dimension 0, may hold values from 0 to 1, as said below
- tile_pattern: int32 [8, 4], P('grp'), parts along dimension 0, may hold values from 0 to 1, as said below
Outputs:
- edges: bfloat16 [512, 1024], P(('grp', 'src'), 'tgt'), parts along dimension 0
The draws below stay inside these ranges and needn't reach their ends.
There are 2 independent parts, one for each index of `grp`. The reference program is written for one: setup_inputs(seed, part) draws one part's arguments, and reference() takes and returns one part's arrays. A program takes and returns all parts, laid end to end along the dimension named above; an argument that names none is the same for every part. Nothing has to cross between parts.
Inputs may be any that keep to these rules, and one draw needn't show every extreme that they name: Each row attention[h, p, :] is a probability distribution over the keys 0 to p: zero beyond p, summing to one. tile_pattern[b, c] is 1 where the tile of edges between source block b and target block c is kept, else 0.
All inputs are finite; a program needn't handle non-finite values.
Results may differ from the reference program's by a relative error of at most 0.0057.
Values may be sent and summed in bfloat16 or wider, within the bound.
A program may use at most 64 MiB of HBM per device.

```python
import jax
import jax.numpy as jnp
from jax import lax

D = 4608
H = 32
KV = 16
HD = 128
S = 256
TGT_DEV = 256
SRC_DEV = 64
BLOCKS = 4
NT = 1024
NS = 256


def draw_attention(key, part):
    noise_key = jax.random.fold_in(key, 11)
    logits = 3.0 * jax.random.normal(noise_key, (H, S, S), jnp.float32)
    query_pos = jnp.arange(S)[:, None]
    key_pos = jnp.arange(S)[None, :]
    causal = key_pos <= query_pos
    logits = jnp.where(causal[None], logits, -1e+30)
    weights = jax.nn.softmax(logits, axis=-1)
    return weights.astype(jnp.bfloat16)


def draw_tile_pattern(key, part):
    level_key, roll_key = jax.random.split(jax.random.fold_in(key, 23))
    levels = jnp.array([6, 12, 25, 50, 100], jnp.int32)
    choose = jax.random.randint(level_key, (BLOCKS,), 0, 5)
    dice_rolls = jax.random.randint(roll_key, (BLOCKS, BLOCKS), 0, 100)
    return (dice_rolls < levels[choose][None, :]).astype(jnp.int32)


def touch_ends(entries, rng, smallest, top_value):
    longest = entries.shape.index(max(entries.shape))
    spots = []
    for shift in (0, 1):
        where = [jax.random.randint(jax.random.fold_in(rng, axis), (), 0, length) for axis, length in enumerate(entries.shape)]
        where[longest] = (where[longest] + shift) % entries.shape[longest]
        spots.append(tuple(where))
    return entries.at[spots[0]].set(smallest).at[spots[1]].set(top_value)


def block_levels(key, shape, cuts, low, high):
    level = 1.0
    for position, shards_of in cuts:
        steps = jax.random.uniform(jax.random.fold_in(jax.random.fold_in(key, 6), position), (shards_of,), jnp.float32, low / len(cuts), high / len(cuts))
        level = level * jnp.repeat(jnp.exp(steps), shape[position] // shards_of).reshape((-1,) + (1,) * (len(shape) - 1 - position))
    return level


def centred(stream_key, shape, deviation, most, pieces=(), held_as=jnp.bfloat16):
    result = deviation * jax.random.normal(stream_key, shape, jnp.float32)
    if pieces:
        result = result * block_levels(stream_key, shape, pieces, -0.22, 0.18)
    return jnp.clip(result, -most, most).astype(held_as)


def setup_inputs(seed: int = 0, part: int = 0) -> dict:
    key_of = jax.random.split(jax.random.key(seed), 9)
    part_keys = jax.random.split(jax.random.fold_in(key_of[8], part), 9)
    return {
        "target_rows": centred(part_keys[0], (NT, D), 1.0, 6.0, ((0, 16),)),
        "target_pos": touch_ends(jax.random.randint(part_keys[1], (NT,), 0, S), jax.random.fold_in(part_keys[1], 1), 0, S - 1).astype(jnp.int32),
        "decoder_rows": centred(part_keys[2], (NS, D), D ** -0.5, 0.09375, ((0, 16),)),
        "source_pos": touch_ends(jax.random.randint(part_keys[3], (NS,), 0, S), jax.random.fold_in(part_keys[3], 1), 0, S - 1).astype(jnp.int32),
        "out_proj": centred(key_of[4], (H, D, HD), D ** -0.5, 0.09375, ((0, 4), (1, 4))),
        "value_proj": centred(key_of[5], (KV, D, HD), (HD // 4) ** -0.5, 1.0, ((0, 4),)),
        "attention": draw_attention(jax.random.fold_in(jax.random.fold_in(key_of[8], part), 71), part),
        "tile_pattern": draw_tile_pattern(jax.random.fold_in(jax.random.fold_in(key_of[8], part), 71), part),
    }


def reference(target_rows, target_pos, decoder_rows, source_pos, out_proj, value_proj, attention, tile_pattern):
    highest = lax.Precision.HIGHEST
    targets_wide = target_rows.astype(jnp.float32)
    sources_wide = decoder_rows.astype(jnp.float32)
    head_reads = jnp.einsum('td,hde->the', targets_wide, out_proj.astype(jnp.float32), precision=highest).astype(jnp.bfloat16)
    source_values = jnp.einsum('nd,gde->nge', sources_wide, value_proj.astype(jnp.float32), precision=highest).astype(jnp.bfloat16)
    same_place = (source_pos[:, None] == target_pos[None, :]).astype(jnp.float32)
    direct = jnp.dot(sources_wide, targets_wide.T, precision=highest) * same_place
    repeat = H // KV

    def add_head(head_index, running):
        group_index = head_index // repeat
        value_part = lax.dynamic_index_in_dim(source_values, group_index, 1, keepdims=False).astype(jnp.float32)
        read_part = lax.dynamic_index_in_dim(head_reads, head_index, 1, keepdims=False).astype(jnp.float32)
        scores = jnp.dot(value_part, read_part.T, precision=highest)
        attn_table = lax.dynamic_index_in_dim(attention, head_index, 0, keepdims=False).astype(jnp.float32)
        weights = jnp.take(jnp.take(attn_table, target_pos, axis=0), source_pos, axis=1).T
        return running + weights * scores

    mixed_term = lax.fori_loop(0, H, add_head, jnp.zeros((NS, NT), jnp.float32))
    keep_mask = jnp.repeat(jnp.repeat(tile_pattern, SRC_DEV, axis=0), TGT_DEV, axis=1).astype(jnp.float32)
    return (keep_mask * (direct + mixed_term)).astype(jnp.bfloat16)
```

```python
import functools

import jax
import jax.numpy as jnp
from jax import lax
from jax.experimental import pallas as pl
from jax.experimental.pallas import tpu as pltpu
from jax.sharding import PartitionSpec as P


def passed_along(value, axis, steps):
    count = lax.axis_size(axis)
    pairs = [(source, (source + steps) % count) for source in range(count)]
    return lax.ppermute(value, axis, pairs)


def gathered_shards(
    target_rows, target_pos, decoder_rows, source_pos, out_proj, value_proj, attention, tile_pattern
):
    blocks = lax.axis_size("tgt")
    column = lax.axis_index("tgt")
    src_lane = lax.axis_index("src")
    full_targets, full_sources = (
        lax.all_gather(target_rows, "src", axis=0, tiled=True),
        lax.all_gather(decoder_rows, "src", axis=0, tiled=True),
    )
    tgt_dev = full_targets.shape[0]
    src_dev = full_sources.shape[0]
    sub_rows = decoder_rows.shape[0]
    heads_here = out_proj.shape[0]
    head_dim = out_proj.shape[2]
    groups_here = value_proj.shape[0]
    repeat = heads_here // groups_here
    read_sum = jnp.einsum(
        "td,hde->the",
        full_targets,
        lax.all_gather(out_proj, "tgt", axis=1, tiled=True),
        preferred_element_type=jnp.float32,
    )
    head_reads = read_sum.astype(jnp.bfloat16).reshape(tgt_dev, groups_here, repeat, head_dim)
    values = jnp.einsum("sd,gde->sge", full_sources, value_proj, preferred_element_type=jnp.float32)
    values = values.astype(jnp.bfloat16).reshape(src_dev, groups_here * head_dim)
    attn_table = lax.all_gather(attention, "tgt", axis=1, tiled=True)
    target_attn = jnp.take(attn_table, target_pos, axis=1)
    keyed_attn = jnp.transpose(target_attn, (0, 2, 1))

    def edge_tile(payload, block_index):
        decoder_part, value_part = payload
        key_positions = lax.dynamic_slice_in_dim(source_pos, block_index * src_dev, src_dev)
        weights = jnp.take(keyed_attn, key_positions, axis=1).astype(jnp.float32)
        scores = jnp.einsum(
            "sgd,tgrd->grst",
            value_part.reshape(src_dev, groups_here, head_dim),
            head_reads,
            preferred_element_type=jnp.float32,
        )
        scores = scores.reshape(heads_here, src_dev, tgt_dev)
        mixed_term = jnp.sum(weights * scores, axis=0)
        own_positions = lax.dynamic_slice_in_dim(key_positions, src_lane * sub_rows, sub_rows)
        same_place = (own_positions[:, None] == target_pos[None, :]).astype(jnp.float32)
        direct = (
            jnp.einsum("sd,td->st", decoder_part, full_targets, preferred_element_type=jnp.float32)
            * same_place
        )
        own_rows = lax.dynamic_slice_in_dim(mixed_term, src_lane * sub_rows, sub_rows, 0)
        return lax.dynamic_update_slice_in_dim(
            mixed_term, own_rows + direct, src_lane * sub_rows, 0
        )

    def place_tile(partial_value, payload, block_index):
        kept_flag = tile_pattern[block_index, column]
        piece_tile = edge_tile(payload, block_index) * kept_flag.astype(jnp.float32)
        return lax.dynamic_update_slice_in_dim(partial_value, piece_tile, block_index * src_dev, 0)

    own_block = (decoder_rows, values)
    partial_value = jnp.zeros((blocks * src_dev, tgt_dev), jnp.float32)
    partial_value = place_tile(partial_value, own_block, column)

    def cycle_turn(turn_index, state_carry):
        forward_block, backward_block, running = state_carry
        forward_block = passed_along((forward_block[0], forward_block[1]), "tgt", 1)
        backward_block = passed_along((backward_block[0], backward_block[1]), "tgt", -1)
        running = place_tile(running, forward_block, (column - turn_index) % blocks)
        running = place_tile(running, backward_block, (column + turn_index) % blocks)
        return (forward_block, backward_block, running)

    forward_block, backward_block, partial_value = lax.fori_loop(
        1, blocks // 2, cycle_turn, (own_block, own_block, partial_value)
    )
    forward_block = passed_along((forward_block[0], forward_block[1]), "tgt", 1)
    partial_value = place_tile(partial_value, forward_block, (column - blocks // 2) % blocks)
    summed = lax.psum_scatter(partial_value, "src", scatter_dimension=0, tiled=True)
    return summed.astype(jnp.bfloat16)


F32 = jnp.float32
BF16 = jnp.bfloat16
MESH = pl.DeviceIdType.MESH


def dot(a, b):
    return jnp.dot(a, b, preferred_element_type=F32)


def dot_nt(a, b):
    return lax.dot_general(a, b, (((1,), (1,)), ((), ())), preferred_element_type=F32)


def edge_kernel(
    nt, ns, tgt_ref, tpos_ref, dec_ref, scol_ref, srow_ref, oproj_hbm, vproj_hbm, attn_ref, pat_ref,
    out_ref,
    oproj, vproj, tslices, dslices, decfull, attn, tpos, values, reads, attn_n, onehot, edges,
    core_in, x_out, x_in, z_out, z_in,
    local_sem, zt_s, zt_r, zd_s, zd_r, zp_s, zp_r, ar_s, al_s, a_r, zv_s, zv_r,
    xt_s, xt_r, ct_s, ct_r, xf_s, xf_r, cf_s, cf_r, ce_s, ce_r, xe_s, xe_r, ze_s, ze_r,
):
    c = lax.axis_index("tgt")
    s = lax.axis_index("src")
    nx = ns // 2
    x = s // 2
    core = s % 2
    mate = x * 2 + 1 - core
    rows, depth = tslices.shape[1] // ns, tslices.shape[2]
    sub = dec_ref.shape[0]
    heads = oproj.shape[0]
    groups = vproj.shape[0]
    block = sub * ns
    queries = attn_ref.shape[1]
    own = edges.shape[1] // ns

    def zdev(k):
        return lax.rem(c + k, nt)

    def xsrc(dx):
        return lax.rem(x + dx, nx) * 2 + core

    sent = []

    def send(src, dst, ssem, rsem, axis, index):
        cp = pltpu.make_async_remote_copy(
            src_ref=src, dst_ref=dst, send_sem=ssem, recv_sem=rsem,
            device_id={axis: index}, device_id_type=MESH,
        )
        cp.start()
        sent.append(cp)

    def arrived(dst, rsem):
        pltpu.make_async_remote_copy(
            src_ref=dst, dst_ref=dst, send_sem=local_sem.at[0], recv_sem=rsem,
            device_id={"src": mate}, device_id_type=MESH,
        ).wait_recv()

    barrier = pltpu.get_barrier_semaphore()
    for k in range(1, nt):
        pl.semaphore_signal(barrier, inc=1, device_id={"tgt": zdev(k)}, device_id_type=MESH)
    for dx in range(1, nx):
        pl.semaphore_signal(barrier, inc=1, device_id={"src": xsrc(dx)}, device_id_type=MESH)
    pl.semaphore_signal(barrier, inc=1, device_id={"src": mate}, device_id_type=MESH)
    fetch_v = pltpu.make_async_copy(vproj_hbm, vproj, local_sem.at[1])
    fetch_o = pltpu.make_async_copy(oproj_hbm, oproj, local_sem.at[2])
    fetch_v.start()
    fetch_o.start()
    pl.semaphore_wait(barrier, nt - 1 + nx - 1 + 1)

    def cols(b):
        return pl.ds(pl.multiple_of(b * depth, 128), depth)

    def trow(lane):
        return pl.ds(pl.multiple_of(lane * rows, rows), rows)

    def drow(lane):
        return pl.ds(pl.multiple_of(lane * sub, sub), sub)

    def qrow(b):
        return pl.ds(pl.multiple_of(b * queries, queries), queries)

    def vrow(b):
        return pl.ds(pl.multiple_of(b * block, block), block)

    def erow(lane):
        return pl.ds(pl.multiple_of(lane * own, own), own)

    for dx in range(1, nx):
        send(dec_ref, decfull.at[drow(s)], xf_s.at[dx], xf_r.at[x], "src", xsrc(dx))
    send(dec_ref, decfull.at[drow(s)], cf_s.at[0], cf_r.at[x], "src", mate)
    for k in range(1, nt):
        b = zdev(k)
        send(tgt_ref.at[:, cols(b)], tslices.at[c, trow(s)], zt_s.at[k], zt_r.at[c], "tgt", b)
        send(dec_ref.at[:, cols(b)], dslices.at[drow(c)], zd_s.at[k], zd_r.at[c], "tgt", b)
        send(tpos_ref, tpos.at[c], zp_s.at[k], zp_r.at[c], "tgt", b)
    for dx in range(1, nx):
        send(tgt_ref.at[:, cols(c)], tslices.at[c, trow(s)], xt_s.at[0, dx], xt_r.at[c, x], "src", xsrc(dx))
    send(tgt_ref.at[:, cols(c)], tslices.at[c, trow(s)], ct_s.at[0, 0], ct_r.at[c, x], "src", mate)

    def to_right(src, b):
        return pltpu.make_async_remote_copy(
            src_ref=src, dst_ref=attn.at[:, qrow(b), :], send_sem=ar_s.at[b], recv_sem=a_r.at[b],
            device_id={"tgt": c + 1}, device_id_type=MESH,
        )

    def to_left(src, b):
        return pltpu.make_async_remote_copy(
            src_ref=src, dst_ref=attn.at[:, qrow(b), :], send_sem=al_s.at[b], recv_sem=a_r.at[b],
            device_id={"tgt": c - 1}, device_id_type=MESH,
        )

    @pl.when(c + 1 < nt)
    def _():
        to_right(attn_ref, c).start()

    @pl.when(c > 0)
    def _():
        to_left(attn_ref, c).start()

    tslices[c, trow(s)] = tgt_ref[:, cols(c)]
    dslices[drow(c)] = dec_ref[:, cols(c)]
    decfull[drow(s)] = dec_ref[...]
    tpos[c] = tpos_ref[...]
    attn[:, qrow(c), :] = attn_ref[...]

    for dx in range(1, nx):
        y = xsrc(dx)
        arrived(decfull.at[drow(y)], xf_r.at[lax.rem(x + dx, nx)])
        send(decfull.at[drow(y)], decfull.at[drow(y)], cf_s.at[dx], cf_r.at[lax.rem(x + dx, nx)], "src", mate)
    for dx in range(nx):
        z = lax.rem(x + dx, nx)
        arrived(decfull.at[drow(z * 2 + 1 - core)], cf_r.at[z])
    fetch_v.wait()

    @pl.loop(0, groups)
    def _(g):
        values[g, vrow(c)] = dot(decfull[...], vproj[g]).astype(BF16)

    fetch_o.wait()

    def pass_rows(k):
        b = zdev(nt - k)
        arrived(tslices.at[b, trow(s)], zt_r.at[b])
        for dx in range(1, nx):
            send(tslices.at[b, trow(s)], tslices.at[b, trow(s)], xt_s.at[k, dx], xt_r.at[b, x], "src", xsrc(dx))
        send(tslices.at[b, trow(s)], tslices.at[b, trow(s)], ct_s.at[k, 0], ct_r.at[b, x], "src", mate)

    def pass_over(k):
        b = zdev(nt - k) if k else c
        for dx in range(1, nx):
            z = lax.rem(x + dx, nx)
            y = z * 2 + core
            arrived(tslices.at[b, trow(y)], xt_r.at[b, z])
            send(tslices.at[b, trow(y)], tslices.at[b, trow(y)], ct_s.at[k, dx], ct_r.at[b, z], "src", mate)

    def read_block(k):
        b = zdev(nt - k) if k else c
        for dx in range(nx):
            z = lax.rem(x + dx, nx)
            arrived(tslices.at[b, trow(z * 2 + 1 - core)], ct_r.at[b, z])

        @pl.loop(0, heads)
        def _(h):
            reads[b, h] = dot(tslices[b], oproj[h]).astype(BF16)

    def relay(k):
        @pl.when(c - k >= 0)
        def _():
            b = c - k
            arrived(attn.at[:, qrow(b), :], a_r.at[b])

            @pl.when(c + 1 < nt)
            def _():
                to_right(attn.at[:, qrow(b), :], b).start()

        @pl.when(c + k < nt)
        def _():
            b = c + k
            arrived(attn.at[:, qrow(b), :], a_r.at[b])

            @pl.when(c > 0)
            def _():
                to_left(attn.at[:, qrow(b), :], b).start()

    for k in range(1, nt):
        send(values.at[:, vrow(c), :], values.at[:, vrow(c), :], zv_s.at[k], zv_r.at[c], "tgt", zdev(k))
    for k in range(1, nt):
        pass_rows(k)
        pass_over(k - 1)
    relay(1)
    read_block(0)
    pass_over(nt - 1)
    for k in range(1, nt):
        if k > 1:
            relay(k)
        read_block(k)
    for k in range(1, nt):
        b = zdev(k)
        arrived(dslices.at[drow(b)], zd_r.at[b])
        arrived(tpos.at[b], zp_r.at[b])
        arrived(values.at[:, vrow(b), :], zv_r.at[b])

    total = scol_ref.shape[0]
    keys = attn.shape[2]
    pick = (scol_ref[...] == lax.broadcasted_iota(jnp.int32, (total, keys), 1)).astype(BF16)

    @pl.loop(0, heads)
    def _(h):
        attn_n[h] = dot_nt(pick, attn[h]).astype(BF16)

    targets = tpos.shape[2]

    def tile(k):
        b = zdev(k + 1)
        here = tpos[b]
        onehot[...] = (lax.broadcasted_iota(jnp.int32, (nt * queries, targets), 0) == here).astype(BF16)
        edges[b] = jnp.zeros(edges.shape[1:], F32)

        @pl.loop(0, heads)
        def _(h):
            weights = dot(attn_n[h], onehot[...])
            scores = dot_nt(values[h // (heads // groups)], reads[b, h])
            edges[b] += weights * scores

        direct = dot_nt(dslices[...], tslices[b])
        for p in range(nt):
            at = pl.ds(pl.multiple_of(p * block + s * sub, sub), sub)
            same = (scol_ref[at] == here).astype(F32)
            edges[b, at] += direct[p * sub:(p + 1) * sub] * same
        for z in range(nx):
            y = z * 2 + 1 - core
            send(edges.at[b, erow(y)], core_in.at[b, z], ce_s.at[k, z], ce_r.at[b, z], "src", mate)

    def over_x(k):
        b = zdev(k + 1)
        for z in range(nx):
            arrived(core_in.at[b, z], ce_r.at[b, z])
        for dx in range(1, nx):
            z = lax.rem(x + dx, nx)
            x_out[b, dx] = (edges[b, erow(z * 2 + core)] + core_in[b, z]).astype(BF16)
            send(x_out.at[b, dx], x_in.at[b, x], xe_s.at[k, dx], xe_r.at[b, x], "src", z * 2 + core)

    def over_z(k):
        b = zdev(k + 1)
        mine = edges[b, erow(s)] + core_in[b, x]
        for dx in range(1, nx):
            z = lax.rem(x + dx, nx)
            arrived(x_in.at[b, z], xe_r.at[b, z])
            mine += x_in[b, z].astype(F32)
        if k < nt - 1:
            z_out[b] = mine.astype(BF16)
            send(z_out.at[b], z_in.at[c], ze_s.at[k], ze_r.at[c], "tgt", b)
        return mine

    for k in range(nt + 2):
        if k < nt:
            tile(k)
        if 0 <= k - 1 < nt:
            over_x(k - 1)
        if 0 <= k - 2 < nt:
            mine = over_z(k - 2)
    for k in range(1, nt):
        b = zdev(k)
        arrived(z_in.at[b], ze_r.at[b])
        mine += z_in[b].astype(F32)
    kept = pat_ref[(s * own) // block, c]
    out_ref[...] = (mine * kept.astype(F32)).astype(BF16)

    for cp in sent:
        cp.wait_send()
    for k in range(nt):
        @pl.when((c - k >= 0) & (c + 1 < nt))
        def _():
            to_right(attn_ref, c - k).wait_send()

        @pl.when((c + k < nt) & (c > 0))
        def _():
            to_left(attn_ref, c + k).wait_send()


def resident_shards(
    target_rows, target_pos, decoder_rows, source_pos, out_proj, value_proj, attention, tile_pattern
):
    nt, ns = lax.axis_size("tgt"), lax.axis_size("src")
    rows = target_rows.shape[0]
    sub, width = decoder_rows.shape
    heads, depth, head_dim = out_proj.shape
    groups = value_proj.shape[0]
    _, queries, keys = attention.shape
    total = source_pos.shape[0]
    targets = target_pos.shape[0]
    own = total // ns
    nx = ns // 2
    vmem = pl.BlockSpec(memory_space=pltpu.VMEM)
    hbm = pl.BlockSpec(memory_space=pl.ANY)
    sem = lambda *shape: pltpu.SemaphoreType.DMA(shape)
    return pl.pallas_call(
        functools.partial(edge_kernel, nt, ns),
        out_shape=jax.ShapeDtypeStruct((own, targets), BF16),
        in_specs=[vmem, vmem, vmem, vmem, vmem, hbm, hbm, vmem, pl.BlockSpec(memory_space=pltpu.SMEM)],
        out_specs=vmem,
        scratch_shapes=[
            pltpu.VMEM(out_proj.shape, BF16),
            pltpu.VMEM(value_proj.shape, BF16),
            pltpu.VMEM((nt, ns * rows, depth), BF16),
            pltpu.VMEM((nt * sub, depth), BF16),
            pltpu.VMEM((ns * sub, width), BF16),
            pltpu.VMEM((heads, nt * queries, keys), BF16),
            pltpu.VMEM((nt, 1, targets), jnp.int32),
            pltpu.VMEM((groups, total, head_dim), BF16),
            pltpu.VMEM((nt, heads, targets, head_dim), BF16),
            pltpu.VMEM((heads, total, nt * queries), BF16),
            pltpu.VMEM((nt * queries, targets), BF16),
            pltpu.VMEM((nt, total, targets), F32),
            pltpu.VMEM((nt, nx, own, targets), F32),
            pltpu.VMEM((nt, nx, own, targets), BF16),
            pltpu.VMEM((nt, nx, own, targets), BF16),
            pltpu.VMEM((nt, own, targets), BF16),
            pltpu.VMEM((nt, own, targets), BF16),
            sem(3),
            sem(nt), sem(nt), sem(nt), sem(nt), sem(nt), sem(nt),
            sem(nt), sem(nt), sem(nt), sem(nt), sem(nt),
            sem(nt, nx), sem(nt, nx), sem(nt, nx), sem(nt, nx),
            sem(nx), sem(nx), sem(nx), sem(nx),
            sem(nt, nx), sem(nt, nx), sem(nt, nx), sem(nt, nx), sem(nt), sem(nt),
        ],
        compiler_params=pltpu.CompilerParams(
            collective_id=0, has_side_effects=True, vmem_limit_bytes=60 * 1024 * 1024
        ),
    )(
        target_rows, target_pos.reshape(1, targets), decoder_rows, source_pos.reshape(total, 1),
        source_pos.reshape(1, total), out_proj, value_proj, attention, tile_pattern,
    )


def resident_bytes(nt, ns, width, heads, depth, groups, rows, total, targets):
    weights = heads * depth * 128 + groups * width * 128
    gathered = nt * ns * rows * depth + nt * heads * targets * 128
    return 2 * (weights + gathered) + 4 * nt * total * targets * 2


def shards(
    target_rows, target_pos, decoder_rows, source_pos, out_proj, value_proj, attention, tile_pattern
):
    nt, ns = lax.axis_size("tgt"), lax.axis_size("src")
    heads, depth, head_dim = out_proj.shape
    need = resident_bytes(
        nt, ns, target_rows.shape[1], heads, depth, value_proj.shape[0], target_rows.shape[0],
        source_pos.shape[0], target_pos.shape[0],
    )
    fits = (
        depth % 128 == 0 and head_dim == 128 and ns % 2 == 0 and nt > 1
        and decoder_rows.shape[0] % 16 == 0 and attention.shape[1] % 16 == 0
        and need < 40 * 1024 * 1024
    )
    plan = resident_shards if fits else gathered_shards
    return plan(
        target_rows, target_pos, decoder_rows, source_pos, out_proj, value_proj, attention, tile_pattern
    )


def solution(mesh):
    return jax.shard_map(
        shards,
        mesh=mesh,
        in_specs=(
            P(("grp", "tgt", "src"), None),
            P(("grp", "tgt")),
            P(("grp", "tgt", "src"), None),
            P("grp"),
            P("src", "tgt", None),
            P("src", None, None),
            P(("grp", "src"), "tgt", None),
            P("grp", None),
        ),
        out_specs=P(("grp", "src"), "tgt"),
        check_vma=False,
    )
```

```python
import functools

import jax
import jax.numpy as jnp
from jax import lax
from jax.experimental import pallas as pl
from jax.experimental.pallas import tpu as pltpu
from jax.sharding import PartitionSpec as P


def passed_along(value, axis, steps):
    count = lax.axis_size(axis)
    pairs = [(source, (source + steps) % count) for source in range(count)]
    return lax.ppermute(value, axis, pairs)


def gathered_shards(
    target_rows, target_pos, decoder_rows, source_pos, out_proj, value_proj, attention, tile_pattern
):
    blocks = lax.axis_size("tgt")
    column = lax.axis_index("tgt")
    src_lane = lax.axis_index("src")
    full_targets, full_sources = (
        lax.all_gather(target_rows, "src", axis=0, tiled=True),
        lax.all_gather(decoder_rows, "src", axis=0, tiled=True),
    )
    tgt_dev = full_targets.shape[0]
    src_dev = full_sources.shape[0]
    sub_rows = decoder_rows.shape[0]
    heads_here = out_proj.shape[0]
    head_dim = out_proj.shape[2]
    groups_here = value_proj.shape[0]
    repeat = heads_here // groups_here
    read_sum = jnp.einsum(
        "td,hde->the",
        full_targets,
        lax.all_gather(out_proj, "tgt", axis=1, tiled=True),
        preferred_element_type=jnp.float32,
    )
    head_reads = read_sum.astype(jnp.bfloat16).reshape(tgt_dev, groups_here, repeat, head_dim)
    values = jnp.einsum("sd,gde->sge", full_sources, value_proj, preferred_element_type=jnp.float32)
    values = values.astype(jnp.bfloat16).reshape(src_dev, groups_here * head_dim)
    attn_table = lax.all_gather(attention, "tgt", axis=1, tiled=True)
    target_attn = jnp.take(attn_table, target_pos, axis=1)
    keyed_attn = jnp.transpose(target_attn, (0, 2, 1))

    def edge_tile(payload, block_index):
        decoder_part, value_part = payload
        key_positions = lax.dynamic_slice_in_dim(source_pos, block_index * src_dev, src_dev)
        weights = jnp.take(keyed_attn, key_positions, axis=1).astype(jnp.float32)
        scores = jnp.einsum(
            "sgd,tgrd->grst",
            value_part.reshape(src_dev, groups_here, head_dim),
            head_reads,
            preferred_element_type=jnp.float32,
        )
        scores = scores.reshape(heads_here, src_dev, tgt_dev)
        mixed_term = jnp.sum(weights * scores, axis=0)
        own_positions = lax.dynamic_slice_in_dim(key_positions, src_lane * sub_rows, sub_rows)
        same_place = (own_positions[:, None] == target_pos[None, :]).astype(jnp.float32)
        direct = (
            jnp.einsum("sd,td->st", decoder_part, full_targets, preferred_element_type=jnp.float32)
            * same_place
        )
        own_rows = lax.dynamic_slice_in_dim(mixed_term, src_lane * sub_rows, sub_rows, 0)
        return lax.dynamic_update_slice_in_dim(
            mixed_term, own_rows + direct, src_lane * sub_rows, 0
        )

    def place_tile(partial_value, payload, block_index):
        kept_flag = tile_pattern[block_index, column]
        piece_tile = edge_tile(payload, block_index) * kept_flag.astype(jnp.float32)
        return lax.dynamic_update_slice_in_dim(partial_value, piece_tile, block_index * src_dev, 0)

    own_block = (decoder_rows, values)
    partial_value = jnp.zeros((blocks * src_dev, tgt_dev), jnp.float32)
    partial_value = place_tile(partial_value, own_block, column)

    def cycle_turn(turn_index, state_carry):
        forward_block, backward_block, running = state_carry
        forward_block = passed_along((forward_block[0], forward_block[1]), "tgt", 1)
        backward_block = passed_along((backward_block[0], backward_block[1]), "tgt", -1)
        running = place_tile(running, forward_block, (column - turn_index) % blocks)
        running = place_tile(running, backward_block, (column + turn_index) % blocks)
        return (forward_block, backward_block, running)

    forward_block, backward_block, partial_value = lax.fori_loop(
        1, blocks // 2, cycle_turn, (own_block, own_block, partial_value)
    )
    forward_block = passed_along((forward_block[0], forward_block[1]), "tgt", 1)
    partial_value = place_tile(partial_value, forward_block, (column - blocks // 2) % blocks)
    summed = lax.psum_scatter(partial_value, "src", scatter_dimension=0, tiled=True)
    return summed.astype(jnp.bfloat16)


F32 = jnp.float32
BF16 = jnp.bfloat16
MESH = pl.DeviceIdType.MESH


def dot(a, b):
    return jnp.dot(a, b, preferred_element_type=F32)


def dot_nt(a, b):
    return lax.dot_general(a, b, (((1,), (1,)), ((), ())), preferred_element_type=F32)


def edge_kernel(
    nt, ns, tgt_ref, tpos_ref, dec_ref, srow_ref, oproj_hbm, vproj_hbm, attn_ref, pat_ref,
    out_ref,
    oproj, vproj, tslices, dslices, decfull, attn, tpos, values, reads, attn_n, onehot, edges,
    core_in, x_out, x_in, z_out, z_in, scol_ref,
    local_sem, zt_s, zt_r, zd_s, zd_r, zp_s, zp_r, ar_s, al_s, a_r, vr_s, vl_s, v_r,
    xt_s, xt_r, ct_s, ct_r, xf_s, xf_r, cf_s, cf_r, ce_s, ce_r, xe_s, xe_r, ze_s, ze_r,
):
    c = lax.axis_index("tgt")
    s = lax.axis_index("src")
    nx = ns // 2
    x = s // 2
    core = s % 2
    mate = x * 2 + 1 - core
    rows, depth = tslices.shape[1] // ns, tslices.shape[2]
    sub = dec_ref.shape[0]
    heads = oproj.shape[0]
    groups = vproj.shape[0]
    block = sub * ns
    queries, keys = attn_ref.shape[1:]
    targets = tpos.shape[2]
    total = scol_ref.shape[0]
    own = edges.shape[1] // ns

    def zdev(k):
        return lax.rem(c + k, nt)

    def xsrc(dx):
        return lax.rem(x + dx, nx) * 2 + core

    def xother(dx):
        return lax.rem(x + dx, nx) * 2 + 1 - core

    sent = []

    def send(src, dst, ssem, rsem, axis, index):
        cp = pltpu.make_async_remote_copy(
            src_ref=src, dst_ref=dst, send_sem=ssem, recv_sem=rsem,
            device_id={axis: index}, device_id_type=MESH,
        )
        cp.start()
        sent.append(cp)

    def arrived(dst, rsem):
        pltpu.make_async_remote_copy(
            src_ref=dst, dst_ref=dst, send_sem=local_sem.at[0], recv_sem=rsem,
            device_id={"src": mate}, device_id_type=MESH,
        ).wait_recv()

    barrier = pltpu.get_barrier_semaphore()
    for k in range(1, nt):
        pl.semaphore_signal(barrier, inc=1, device_id={"tgt": zdev(k)}, device_id_type=MESH)
    for dx in range(1, nx):
        pl.semaphore_signal(barrier, inc=1, device_id={"src": xsrc(dx)}, device_id_type=MESH)
        pl.semaphore_signal(barrier, inc=1, device_id={"src": xother(dx)}, device_id_type=MESH)
    pl.semaphore_signal(barrier, inc=1, device_id={"src": mate}, device_id_type=MESH)
    fetch_v = pltpu.make_async_copy(vproj_hbm, vproj, local_sem.at[1])
    fetch_o = pltpu.make_async_copy(oproj_hbm, oproj, local_sem.at[2])
    fetch_v.start()
    fetch_o.start()
    pl.semaphore_wait(barrier, nt - 1 + ns - 1)

    def cols(b):
        return pl.ds(pl.multiple_of(b * depth, 128), depth)

    def trow(lane):
        return pl.ds(pl.multiple_of(lane * rows, rows), rows)

    def drow(lane):
        return pl.ds(pl.multiple_of(lane * sub, sub), sub)

    def qrow(b):
        return pl.ds(pl.multiple_of(b * queries, queries), queries)

    def vrow(b):
        return pl.ds(pl.multiple_of(b * block, block), block)

    def erow(lane):
        return pl.ds(pl.multiple_of(lane * own, own), own)

    for dx in range(1, nx):
        send(dec_ref, decfull.at[drow(s)], xf_s.at[dx], xf_r.at[x], "src", xsrc(dx))
    send(dec_ref, decfull.at[drow(s)], cf_s.at[0], cf_r.at[x], "src", mate)
    def spread(k):
        b = zdev(k)
        send(tgt_ref.at[:, cols(b)], tslices.at[c, trow(s)], zt_s.at[k], zt_r.at[c], "tgt", b)
        send(dec_ref.at[:, cols(b)], dslices.at[drow(c)], zd_s.at[k], zd_r.at[c], "tgt", b)
        send(tpos_ref, tpos.at[c], zp_s.at[k], zp_r.at[c], "tgt", b)

    for dx in range(1, nx):
        send(tgt_ref.at[:, cols(c)], tslices.at[c, trow(s)], xt_s.at[0, dx], xt_r.at[c, x], "src", xsrc(dx))
    send(tgt_ref.at[:, cols(c)], tslices.at[c, trow(s)], ct_s.at[0, 0], ct_r.at[c, x], "src", mate)

    half = keys // 2
    lowest = half // queries if half % 128 == 0 else 0

    def attn_copy(src, b, ssem, device, act):
        @pl.when(b < lowest)
        def _():
            act(pltpu.make_async_remote_copy(
                src_ref=src.at[:, :, pl.ds(0, half)], dst_ref=attn.at[:, qrow(b), pl.ds(0, half)],
                send_sem=ssem.at[b], recv_sem=a_r.at[b],
                device_id={"tgt": device}, device_id_type=MESH,
            ))

        @pl.when(b >= lowest)
        def _():
            act(pltpu.make_async_remote_copy(
                src_ref=src, dst_ref=attn.at[:, qrow(b), :],
                send_sem=ssem.at[b], recv_sem=a_r.at[b],
                device_id={"tgt": device}, device_id_type=MESH,
            ))

    def value_copy(b, ssem, device):
        return pltpu.make_async_remote_copy(
            src_ref=values.at[:, vrow(b), :], dst_ref=values.at[:, vrow(b), :],
            send_sem=ssem.at[b], recv_sem=v_r.at[b],
            device_id={"tgt": device}, device_id_type=MESH,
        )

    start = lambda copy: copy.start()
    wait_send = lambda copy: copy.wait_send()
    wait_recv = lambda copy: copy.wait_recv()

    @pl.when(c + 1 < nt)
    def _():
        attn_copy(attn_ref, c, ar_s, c + 1, start)

    @pl.when(c > 0)
    def _():
        attn_copy(attn_ref, c, al_s, c - 1, start)

    spread(1)
    spread(2)

    for b in range(lowest):
        attn[:, b * queries:(b + 1) * queries, half:] = jnp.zeros((heads, queries, keys - half), BF16)
    scol_ref[...] = jnp.transpose(jnp.broadcast_to(srow_ref[...], (128, total)))[:, :1]
    tslices[c, trow(s)] = tgt_ref[:, cols(c)]
    dslices[drow(c)] = dec_ref[:, cols(c)]
    decfull[drow(s)] = dec_ref[...]
    tpos[c] = tpos_ref[...]
    attn[:, qrow(c), :] = attn_ref[...]

    for dx in range(1, nx):
        y = xsrc(dx)
        arrived(decfull.at[drow(y)], xf_r.at[lax.rem(x + dx, nx)])
        send(decfull.at[drow(y)], decfull.at[drow(y)], cf_s.at[dx], cf_r.at[lax.rem(x + dx, nx)], "src", mate)
    for dx in range(nx):
        z = lax.rem(x + dx, nx)
        arrived(decfull.at[drow(z * 2 + 1 - core)], cf_r.at[z])
    fetch_v.wait()

    @pl.loop(0, groups)
    def _(g):
        values[g, vrow(c)] = dot(decfull[...], vproj[g]).astype(BF16)

    @pl.when(c + 1 < nt)
    def _():
        value_copy(c, vr_s, c + 1).start()

    @pl.when(c > 0)
    def _():
        value_copy(c, vl_s, c - 1).start()

    fetch_o.wait()

    def pass_rows(k):
        b = zdev(nt - k)
        arrived(tslices.at[b, trow(s)], zt_r.at[b])
        for dx in range(1, nx):
            send(tslices.at[b, trow(s)], tslices.at[b, trow(s)], xt_s.at[k, dx], xt_r.at[b, x], "src", xsrc(dx))
        send(tslices.at[b, trow(s)], tslices.at[b, trow(s)], ct_s.at[k, 0], ct_r.at[b, x], "src", mate)

    def pass_over(k):
        b = zdev(nt - k) if k else c
        for dx in range(1, nx):
            z = lax.rem(x + dx, nx)
            y = z * 2 + core
            arrived(tslices.at[b, trow(y)], xt_r.at[b, z])
            send(tslices.at[b, trow(y)], tslices.at[b, trow(y)], ct_s.at[k, dx], ct_r.at[b, z], "src", mate)

    def read_block(k):
        b = zdev(nt - k) if k else c
        for dx in range(nx):
            z = lax.rem(x + dx, nx)
            arrived(tslices.at[b, trow(z * 2 + 1 - core)], ct_r.at[b, z])

        @pl.loop(0, heads)
        def _(h):
            reads[b, h] = dot(tslices[b], oproj[h]).astype(BF16)

    def relay(k, copy_in, copy_on):
        @pl.when(c - k >= 0)
        def _():
            copy_in(c - k)

            @pl.when(c + 1 < nt)
            def _():
                copy_on(c - k, 0)

        @pl.when(c + k < nt)
        def _():
            copy_in(c + k)

            @pl.when(c > 0)
            def _():
                copy_on(c + k, 1)

    def attn_in(b):
        attn_copy(attn.at[:, qrow(b), :], b, ar_s, c, wait_recv)

    def attn_on(b, left):
        attn_copy(attn.at[:, qrow(b), :], b, al_s if left else ar_s, c - 1 if left else c + 1, start)

    def value_in(b):
        value_copy(b, vr_s, c).wait_recv()

    def value_on(b, left):
        value_copy(b, vl_s if left else vr_s, c - 1 if left else c + 1).start()

    def prepare(k):
        b = zdev(nt - k) if k else c
        if k:
            arrived(dslices.at[drow(b)], zd_r.at[b])
            arrived(tpos.at[b], zp_r.at[b])
        onehot[b] = (
            lax.broadcasted_iota(jnp.int32, (nt * queries, targets), 0) == tpos[b]
        ).astype(BF16)
        edges[b] = jnp.zeros(edges.shape[1:], F32)

    def add_direct(b):
        here = tpos[b]
        direct = dot_nt(dslices[...], tslices[b])
        for p in range(nt):
            at = pl.ds(pl.multiple_of(p * block + s * sub, sub), sub)
            same = (scol_ref[at] == here).astype(F32)
            edges[b, at] += direct[p * sub:(p + 1) * sub] * same

    def pick_keys():
        pick = (scol_ref[...] == lax.broadcasted_iota(jnp.int32, (total, keys), 1)).astype(BF16)

        @pl.loop(0, heads)
        def _(h):
            attn_n[h] = dot_nt(pick, attn[h]).astype(BF16)

    def tile(k):
        b = zdev(nt - 1 - k)
        repeat = heads // groups

        @pl.loop(0, groups)
        def _(g):
            terms = None
            for r in range(repeat):
                h = g * repeat + r
                term = dot(attn_n[h], onehot[b]) * dot_nt(values[g], reads[b, h])
                terms = term if terms is None else terms + term
            edges[b] += terms

        send(edges.at[b, erow(mate)], core_in.at[b], ce_s.at[k], ce_r.at[b], "src", mate)
        for dx in range(1, nx):
            for y in (xsrc(dx), xother(dx)):
                x_out[b, y] = edges[b, erow(y)].astype(BF16)
                send(x_out.at[b, y], x_in.at[b, s], xe_s.at[k, y], xe_r.at[b, s], "src", y)

    def over_z(k):
        b = zdev(nt - 1 - k)
        arrived(core_in.at[b], ce_r.at[b])
        mine = edges[b, erow(s)] + core_in[b]
        for dx in range(1, nx):
            for y in (xsrc(dx), xother(dx)):
                arrived(x_in.at[b, y], xe_r.at[b, y])
                mine += x_in[b, y].astype(F32)
        if k < nt - 1:
            z_out[b] = mine.astype(BF16)
            send(z_out.at[b], z_in.at[c], ze_s.at[k], ze_r.at[c], "tgt", b)
        return mine

    prepare(0)
    for k in range(1, nt):
        relay(k, attn_in, attn_on)
        if k == 1:
            for j in range(3, nt):
                spread(j)
        relay(k, value_in, value_on)
        if k == nt - 1:
            pick_keys()
        pass_rows(k)
        pass_over(k - 1)
        prepare(k)
        if k == 1:
            read_block(0)
    for k in range(1, nt + 2):
        if k < nt:
            read_block(k)
            add_direct(zdev(nt - k))
            tile(k - 1)
        if k == 1:
            pass_over(nt - 1)
        if k == nt:
            add_direct(c)
            tile(k - 1)
        if k > 1:
            mine = over_z(k - 2)
    for k in range(1, nt):
        b = zdev(k)
        arrived(z_in.at[b], ze_r.at[b])
        mine += z_in[b].astype(F32)
    kept = pat_ref[(s * own) // block, c]
    out_ref[...] = (mine * kept.astype(F32)).astype(BF16)

    for cp in sent:
        cp.wait_send()
    for k in range(nt):
        @pl.when((c - k >= 0) & (c + 1 < nt))
        def _():
            attn_copy(attn_ref, c - k, ar_s, c + 1, wait_send)
            value_copy(c - k, vr_s, c + 1).wait_send()

        @pl.when((c + k < nt) & (c > 0))
        def _():
            attn_copy(attn_ref, c + k, al_s, c - 1, wait_send)
            value_copy(c + k, vl_s, c - 1).wait_send()


def resident_shards(
    target_rows, target_pos, decoder_rows, source_pos, out_proj, value_proj, attention, tile_pattern
):
    nt, ns = lax.axis_size("tgt"), lax.axis_size("src")
    rows = target_rows.shape[0]
    sub, width = decoder_rows.shape
    heads, depth, head_dim = out_proj.shape
    groups = value_proj.shape[0]
    _, queries, keys = attention.shape
    total = source_pos.shape[0]
    targets = target_pos.shape[0]
    own = total // ns
    nx = ns // 2
    vmem = pl.BlockSpec(memory_space=pltpu.VMEM)
    hbm = pl.BlockSpec(memory_space=pl.ANY)
    sem = lambda *shape: pltpu.SemaphoreType.DMA(shape)
    return pl.pallas_call(
        functools.partial(edge_kernel, nt, ns),
        out_shape=jax.ShapeDtypeStruct((own, targets), BF16),
        in_specs=[vmem, vmem, vmem, vmem, hbm, hbm, vmem, pl.BlockSpec(memory_space=pltpu.SMEM)],
        out_specs=vmem,
        scratch_shapes=[
            pltpu.VMEM(out_proj.shape, BF16),
            pltpu.VMEM(value_proj.shape, BF16),
            pltpu.VMEM((nt, ns * rows, depth), BF16),
            pltpu.VMEM((nt * sub, depth), BF16),
            pltpu.VMEM((ns * sub, width), BF16),
            pltpu.VMEM((heads, nt * queries, keys), BF16),
            pltpu.VMEM((nt, 1, targets), jnp.int32),
            pltpu.VMEM((groups, total, head_dim), BF16),
            pltpu.VMEM((nt, heads, targets, head_dim), BF16),
            pltpu.VMEM((heads, total, nt * queries), BF16),
            pltpu.VMEM((nt, nt * queries, targets), BF16),
            pltpu.VMEM((nt, total, targets), F32),
            pltpu.VMEM((nt, own, targets), F32),
            pltpu.VMEM((nt, ns, own, targets), BF16),
            pltpu.VMEM((nt, ns, own, targets), BF16),
            pltpu.VMEM((nt, own, targets), BF16),
            pltpu.VMEM((nt, own, targets), BF16),
            pltpu.VMEM((total, 1), jnp.int32),
            sem(3),
            sem(nt), sem(nt), sem(nt), sem(nt), sem(nt), sem(nt),
            sem(nt), sem(nt), sem(nt), sem(nt), sem(nt), sem(nt),
            sem(nt, nx), sem(nt, nx), sem(nt, nx), sem(nt, nx),
            sem(nx), sem(nx), sem(nx), sem(nx),
            sem(nt), sem(nt), sem(nt, ns), sem(nt, ns), sem(nt), sem(nt),
        ],
        compiler_params=pltpu.CompilerParams(
            collective_id=0, has_side_effects=True, vmem_limit_bytes=60 * 1024 * 1024
        ),
    )(
        target_rows, target_pos.reshape(1, targets), decoder_rows, source_pos.reshape(1, total),
        out_proj, value_proj, attention, tile_pattern,
    )


def resident_bytes(nt, ns, width, heads, depth, groups, rows, total, targets):
    weights = heads * depth * 128 + groups * width * 128
    gathered = nt * ns * rows * depth + nt * heads * targets * 128
    return 2 * (weights + gathered) + 4 * nt * total * targets * 2


def shards(
    target_rows, target_pos, decoder_rows, source_pos, out_proj, value_proj, attention, tile_pattern
):
    nt, ns = lax.axis_size("tgt"), lax.axis_size("src")
    heads, depth, head_dim = out_proj.shape
    need = resident_bytes(
        nt, ns, target_rows.shape[1], heads, depth, value_proj.shape[0], target_rows.shape[0],
        source_pos.shape[0], target_pos.shape[0],
    )
    fits = (
        depth % 128 == 0 and head_dim == 128 and ns % 2 == 0 and nt > 2
        and decoder_rows.shape[0] % 16 == 0 and attention.shape[1] % 16 == 0
        and need < 40 * 1024 * 1024
    )
    plan = resident_shards if fits else gathered_shards
    return plan(
        target_rows, target_pos, decoder_rows, source_pos, out_proj, value_proj, attention, tile_pattern
    )


def solution(mesh):
    return jax.shard_map(
        shards,
        mesh=mesh,
        in_specs=(
            P(("grp", "tgt", "src"), None),
            P(("grp", "tgt")),
            P(("grp", "tgt", "src"), None),
            P("grp"),
            P("src", "tgt", None),
            P("src", None, None),
            P(("grp", "src"), "tgt", None),
            P("grp", None),
        ),
        out_specs=P(("grp", "src"), "tgt"),
        check_vma=False,
    )
```
